32 devices in a mesh: sfc: 8 (over z, y), sub: 4 (over x, core).
Axes of the slice: x: 2, y: 2, z: 4, core: 2. Of those that a mesh axis runs over, the one named last changes fastest.
Arguments:
- vectors: float32 [64, 512, 256], P(None, ('sfc', 'sub')), may hold values from -10 to 10
- reaction: float32 [512, 256], P(('sfc', 'sub')), may hold values from 0.5 to 5
Outputs:
- basis: float32 [64, 512, 256], P(None, ('sfc', 'sub'))
- upper: float32 [64, 64], replicated
The draws below stay inside these ranges and needn't reach their ends.
All inputs are finite; a program needn't handle non-finite values.
Results may differ from the reference program's by a relative error of at most 0.0003.
Values sent between devices are 32-bit elements; how exact they have to be, the bound alone decides.
A program may use at most 64 MiB of HBM per device.

```python
import math
import jax
import jax.numpy as jnp
from jax import lax

K = 64
NY = 32
NL = 8
POWERS = 3
PLANE = 256
NX = 512


def draw_vectors(key, part):
    key_shared, key_mixing, key_separate, key_ranking = jax.random.split(jax.random.fold_in(key, 71), 4)
    shared_count = 4
    smallest = 0.01
    shared = jax.random.normal(key_shared, (shared_count, NX, PLANE), jnp.float32)
    separate = jax.random.normal(key_separate, (K, NX, PLANE), jnp.float32)
    mixing = jax.random.normal(key_mixing, (shared_count, K), jnp.float32)
    ranking = jax.random.permutation(key_ranking, K).astype(jnp.float32)
    column_scale = jnp.power(jnp.float32(smallest), ranking / (K - 1))
    common = jnp.einsum('rk,rxp->kxp', mixing, shared) / math.sqrt(shared_count)
    combined = common + column_scale[:, None, None] * separate
    return jnp.clip(combined, -10.0, 10.0).astype(jnp.float32)


def block_scale(own_key, dims, pieces, least, top_value):
    level = 1.0
    for dim, blocks in pieces:
        steps = jax.random.uniform(jax.random.fold_in(jax.random.fold_in(own_key, 6), dim), (blocks,), jnp.float32, least / len(pieces), top_value / len(pieces))
        level = level * jnp.repeat(jnp.exp(steps), dims[dim] // blocks).reshape((-1,) + (1,) * (len(dims) - 1 - dim))
    return level


def setup_inputs(seed: int = 0) -> dict:
    arg_keys = jax.random.split(jax.random.key(seed), 3)
    return {
        "vectors": draw_vectors(jax.random.fold_in(arg_keys[2], 71), 0),
        "reaction": jnp.clip(jnp.exp(math.log(5.0) - 2.3025851 * jax.random.uniform(arg_keys[1], (NX, PLANE), jnp.float32) ** block_scale(arg_keys[1], (NX, PLANE), ((0, 32),), -0.2, 0.2)), 0.5, 5.0),
    }


DELTA_MASS = 0.5

def line_tables(count):
    index = jnp.arange(count)
    offset = index[:, None] - index[None, :]
    near = (jnp.abs(offset) == 1).astype(jnp.float32)
    same = (offset == 0).astype(jnp.float32)
    mass = (4.0 * same + near) / 6.0
    stiff = 2.0 * same - near
    return (mass, stiff)

def tables(across, layers):
    mass_across, stiff_across = line_tables(across)
    mass_layers, stiff_layers = line_tables(layers)
    mass_plane = jnp.kron(mass_layers, mass_across)
    stiff_plane = jnp.kron(mass_layers, stiff_across) + jnp.kron(stiff_layers, mass_across) + DELTA_MASS * mass_plane
    return jnp.concatenate([mass_plane, stiff_plane], axis=1)

def operate(field, reaction, table):
    plane = table.shape[0]
    both = jnp.einsum('kzp,pq->kzq', field, table, precision=lax.Precision.HIGHEST)
    massed = both[..., :plane]
    mixed = both[..., plane:]
    edge_term = mixed / 6.0 - massed
    padded = jnp.pad(edge_term, ((0, 0), (1, 1), (0, 0)))
    return padded[:, :-2] + padded[:, 2:] + 4.0 / 6.0 * mixed + 2.0 * massed + reaction[None] * field

def lower_solve(lower, block):
    return lax.linalg.triangular_solve(lower, block, left_side=True, lower=True)

def reference(vectors, reaction):
    table = tables(NY, NL)
    groups = vectors.reshape(K // 8, 8, NX, NY * NL)

    def power(group):
        field = group
        for _ in range(POWERS):
            field = operate(field, reaction, table)
        return field
    applied = lax.map(power, groups).reshape(K, NX * NY * NL)
    gram = jnp.dot(applied, applied.T, precision=lax.Precision.HIGHEST)
    lower_one = jnp.linalg.cholesky(gram)
    first = lower_solve(lower_one, applied)
    gram_two = jnp.dot(first, first.T, precision=lax.Precision.HIGHEST)
    lower_two = jnp.linalg.cholesky(gram_two)
    second = lower_solve(lower_two, first)
    scale = math.sqrt(NX * NY * NL)
    upper = jnp.dot(lower_one, lower_two, precision=lax.Precision.HIGHEST).T / scale
    return ((second * scale).reshape(K, NX, NY * NL), upper)
```

```python
import functools
import math

import jax
import jax.numpy as jnp
import numpy as np
from jax import lax
from jax.experimental import pallas as pl
from jax.experimental.pallas import tpu as pltpu
from jax.sharding import PartitionSpec as P

NY = 32
NL = 8
POWERS = 3

MESH = pl.DeviceIdType.MESH
F32 = jnp.float32
BF16 = jnp.bfloat16
STEP = 4
LANES = 128


def plane_table(across, layers):
    def near(n):
        return np.eye(n, k=1) + np.eye(n, k=-1)

    one_a, one_l = np.eye(across), np.eye(layers)
    same = np.kron(one_l, one_a)
    side = np.kron(one_l, near(across)) + np.kron(near(layers), one_a)
    corner = np.kron(near(layers), near(across))
    edge = 16.0 * same - 68.0 * side - 35.0 * corner
    own = 304.0 * same + 4.0 * side - 17.0 * corner
    return np.concatenate([edge, own], axis=1)


def split3(x):
    high = x.astype(BF16)
    rest = x - high.astype(F32)
    mid = rest.astype(BF16)
    low = (rest - mid.astype(F32)).astype(BF16)
    return high, mid, low


def loop(count, body):
    if count <= 16:
        for i in range(count):
            body(i)
    else:
        lax.fori_loop(0, count, lambda i, c: (body(i), c)[1], 0)


def gram_of(slabs):
    k = slabs[0].shape[0]
    wide = jnp.concatenate([jnp.concatenate(split3(s), axis=0) for s in slabs], axis=1)
    pairs = lax.dot_general(wide, wide, (((1,), (1,)), ((), ())), preferred_element_type=F32)
    total = None
    for i in (2, 1, 0):
        for j in (2, 1, 0):
            term = pairs[i * k : (i + 1) * k, j * k : (j + 1) * k]
            total = term if total is None else total + term
    return total


def left_parts(matrix):
    a, b, c = split3(matrix)
    return jnp.concatenate([a, a, a, b, b, c], axis=1)


def left_apply(parts, slab):
    a, b, c = split3(slab)
    stacked = jnp.concatenate([a, b, c, a, b, a], axis=0)
    return jnp.dot(parts, stacked, preferred_element_type=F32)


def eliminate(gram):
    k = gram.shape[0]
    rows = lax.broadcasted_iota(jnp.int32, (k, 2 * k), 0)
    cols = lax.broadcasted_iota(jnp.int32, (k, 2 * k), 1)
    unit = (rows + k == cols).astype(F32)
    work = jnp.concatenate([gram, unit[:, k:]], axis=1)
    for start in range(0, k, STEP):
        base = start // 8 * 8
        done, live = work[:base], work[base:]
        live_rows = rows[base:]
        n = live.shape[0]
        columns = [jnp.broadcast_to(live[:, start + i : start + i + 1], (n, 2 * k)) for i in range(STEP)]
        for i in range(STEP):
            j = start + i
            at = j - base
            pivot = columns[i][at : at + 1, :]
            factor = jnp.where(live_rows > j, columns[i] * (1.0 / pivot), 0.0)
            for later in range(i + 1, STEP):
                columns[later] = columns[later] - factor * columns[later][at : at + 1, :]
            live = live - factor * live[at : at + 1, :]
        work = live if base == 0 else jnp.concatenate([done, live], axis=0)
    diagonal = jnp.sum(jnp.where(rows == cols, work, 0.0), axis=1, keepdims=True)
    root = lax.rsqrt(diagonal)
    root = root * (1.5 - 0.5 * diagonal * root * root)
    upper = jnp.where(cols >= rows, work, 0.0)[:, :k] * (1.0 / (diagonal * root))
    inverse = work[:, k:] * root
    return upper, inverse


def pack(gram):
    half = gram.shape[0] // 2
    return jnp.concatenate([gram[:half], gram[half:]], axis=1)


def unpack(packed):
    k = packed.shape[1] // 2
    return jnp.concatenate([packed[:, :k], packed[:, k:]], axis=0)


def gather_sum(axis, box, send_sem, recv_sem, value):
    count = lax.axis_size(axis)
    me = lax.axis_index(axis)
    box[me] = value

    def copy(i, slot, target):
        return pltpu.make_async_remote_copy(
            src_ref=box.at[slot],
            dst_ref=box.at[slot],
            send_sem=send_sem.at[i],
            recv_sem=recv_sem.at[slot],
            device_id={axis: target},
            device_id_type=MESH,
        )

    def start(i):
        copy(i, me, lax.rem(me + i + 1, count)).start()

    def take(i):
        other = lax.rem(me + i + 1, count)
        copy(i, other, other).wait_recv()

    def sent(i):
        copy(i, me, lax.rem(me + i + 1, count)).wait_send()

    loop(count - 1, start)
    loop(count - 1, take)
    if count <= 16:
        total = box[0]
        for i in range(1, count):
            total = total + box[i]
    else:
        total = lax.fori_loop(1, count, lambda i, t: t + box[i], box[0])
    return total, lambda: loop(count - 1, sent)


def main_kernel(
    vec_ref, react_ref, table_ref, q_ref, upper_ref, gram_ref,
    raw, react, fields, edges, send_l, send_r, from_l, from_r,
    box_sub1, box_sfc1, box_sub2, box_sfc2,
    in_sem, halo_send, halo_recv,
    ss1, rs1, sf1, rf1, ss2, rs2, sf2, rf2,
):
    width = POWERS
    n_sfc, n_sub = lax.axis_size("sfc"), lax.axis_size("sub")
    p_sfc, p_sub = lax.axis_index("sfc"), lax.axis_index("sub")
    me = p_sfc * n_sub + p_sub
    last = n_sfc * n_sub - 1
    k, nx, plane = vec_ref.shape

    lanes = raw.shape[-1]
    loads = [
        pltpu.make_async_copy(vec_ref.at[:, :, pl.ds(i * lanes, lanes)], raw.at[i], in_sem.at[i])
        for i in range(plane // lanes)
    ]
    loads.append(
        pltpu.make_async_copy(react_ref, react.at[pl.ds(8, nx)], in_sem.at[plane // lanes])
    )
    for load in loads:
        load.start()

    def device(index):
        return (lax.div(index, n_sub), lax.rem(index, n_sub))

    has_left, has_right = me > 0, me < last
    barrier = pltpu.get_barrier_semaphore()

    def greet(axis, count, mine):
        def one(i):
            pl.semaphore_signal(
                barrier, inc=1, device_id={axis: lax.rem(mine + i + 1, count)}, device_id_type=MESH
            )

        loop(count - 1, one)

    @pl.when(has_left)
    def _():
        pl.semaphore_signal(barrier, inc=1, device_id=device(me - 1), device_id_type=MESH)

    @pl.when(has_right)
    def _():
        pl.semaphore_signal(barrier, inc=1, device_id=device(me + 1), device_id_type=MESH)

    greet("sub", n_sub, p_sub)
    greet("sfc", n_sfc, p_sfc)

    for load in loads:
        load.wait()
    flats = [raw.at[i].reshape(k * nx, lanes) for i in range(plane // lanes)]

    def slab(x):
        return jnp.concatenate([flat[pl.ds(x, k, stride=nx), :] for flat in flats], axis=1)

    halo = width * k
    for i in range(width):
        send_l[pl.ds(i * k, k), :] = slab(i)
        send_r[pl.ds(i * k, k), :] = slab(nx - width + i)
    send_l[pl.ds(halo, 8), :] = react[pl.ds(8, 8), :]
    send_r[pl.ds(halo, 8), :] = react[pl.ds(nx, 8), :]
    for x in range(nx):
        fields[0, width + x] = slab(x)

    pl.semaphore_wait(
        barrier, (n_sub - 1) + (n_sfc - 1) + jnp.minimum(me, 1) + jnp.minimum(last - me, 1)
    )

    def to_left():
        return pltpu.make_async_remote_copy(
            src_ref=send_l, dst_ref=from_r, send_sem=halo_send.at[0], recv_sem=halo_recv.at[1],
            device_id=device(me - 1), device_id_type=MESH,
        )

    def to_right():
        return pltpu.make_async_remote_copy(
            src_ref=send_r, dst_ref=from_l, send_sem=halo_send.at[1], recv_sem=halo_recv.at[0],
            device_id=device(me + 1), device_id_type=MESH,
        )

    @pl.when(has_left)
    def _():
        to_left().start()

    @pl.when(has_right)
    def _():
        to_right().start()

    table = table_ref[...]

    def products(p, lo, hi):
        v = fields[p, width + lo : width + hi].reshape((hi - lo) * k, plane)
        a, b, c = split3(v)
        both = (
            jnp.dot(a, table, preferred_element_type=F32)
            + jnp.dot(b, table, preferred_element_type=F32)
            + jnp.dot(c, table, preferred_element_type=F32)
        )
        edges[p, width + lo : width + hi] = (both[:, :plane] * (1.0 / 432.0)).reshape(hi - lo, k, plane)
        own = both[:, plane:] * (1.0 / 108.0)
        gain = react[8 + lo : 8 + hi, :][:, None, :]
        fields[p + 1, width + lo : width + hi] = own.reshape(hi - lo, k, plane) + gain * v.reshape(hi - lo, k, plane)

    def combine(p, x):
        fields[p + 1, width + x] = (
            fields[p + 1, width + x] + edges[p, width + x - 1] + edges[p, width + x + 1]
        )

    for p in range(width):
        products(p, p, nx - p)
        for x in range(p + 1, nx - p - 1):
            combine(p, x)
    inner = gram_of([fields[width, width + x] for x in range(width, nx - width)])

    zero = jnp.zeros((halo + 8, plane), F32)

    @pl.when(has_left)
    def _():
        to_right_in = pltpu.make_async_remote_copy(
            src_ref=send_r, dst_ref=from_l, send_sem=halo_send.at[1], recv_sem=halo_recv.at[0],
            device_id=device(me - 1), device_id_type=MESH,
        )
        to_right_in.wait_recv()

    @pl.when(jnp.logical_not(has_left))
    def _():
        from_l[...] = zero

    @pl.when(has_right)
    def _():
        to_left_in = pltpu.make_async_remote_copy(
            src_ref=send_l, dst_ref=from_r, send_sem=halo_send.at[0], recv_sem=halo_recv.at[1],
            device_id=device(me + 1), device_id_type=MESH,
        )
        to_left_in.wait_recv()

    @pl.when(jnp.logical_not(has_right))
    def _():
        from_r[...] = zero

    for i in range(width):
        fields[0, i] = from_l[pl.ds(i * k, k), :]
        fields[0, width + nx + i] = from_r[pl.ds(i * k, k), :]
    react[pl.ds(0, 8), :] = from_l[pl.ds(halo, 8), :]
    react[pl.ds(8 + nx, 8), :] = from_r[pl.ds(halo, 8), :]

    keep_left = jnp.where(has_left, 1.0, 0.0).astype(F32)
    keep_right = jnp.where(has_right, 1.0, 0.0).astype(F32)
    for p in range(width):
        products(p, p - width, p)
        products(p, nx - p, nx - p + width)
        for x in range(p - width + 1, p + 1):
            combine(p, x)
            mirror = nx - 1 - x
            combine(p, mirror)
            if x < 0:
                fields[p + 1, width + x] = fields[p + 1, width + x] * keep_left
                fields[p + 1, width + mirror] = fields[p + 1, width + mirror] * keep_right

    outer_rows = list(range(width)) + list(range(nx - width, nx))
    gram = inner + gram_of([fields[width, width + x] for x in outer_rows])

    def reduce(gram, box_sub, ss, rs, box_sfc, sf, rf):
        part, sent_a = gather_sum("sub", box_sub, ss, rs, pack(gram))
        total, sent_b = gather_sum("sfc", box_sfc, sf, rf, part)
        return total, (sent_a, sent_b)

    total, sent1 = reduce(gram, box_sub1, ss1, rs1, box_sfc1, sf1, rf1)
    upper, inverse = eliminate(unpack(total))
    upper_ref[...] = upper
    parts = left_parts(inverse)
    for x in range(nx):
        q_ref[x] = left_apply(parts, fields[width, width + x])
    gram = gram_of([q_ref[x] for x in range(nx)])
    total, sent2 = reduce(gram, box_sub2, ss2, rs2, box_sfc2, sf2, rf2)
    gram_ref[...] = total

    for done in sent1 + sent2:
        done()

    @pl.when(has_left)
    def _():
        to_left().wait_send()

    @pl.when(has_right)
    def _():
        to_right().wait_send()


def last_kernel(scale, q_ref, upper_ref, gram_ref, basis_ref, out_upper_ref, wide, sems):
    nx, k, plane = q_ref.shape
    second, inverse = eliminate(unpack(gram_ref[...]))
    parts = left_parts(inverse * scale)
    pieces = wide.shape[0]
    flats = [wide.at[i].reshape(k * nx, LANES) for i in range(pieces)]
    copies = []
    for x in range(nx):
        slab = left_apply(parts, q_ref[x])
        for i in range(pieces):
            flats[i][pl.ds(x, k, stride=nx), :] = slab[:, i * LANES : (i + 1) * LANES]
        if x % 8 == 7:
            rows = pl.ds(x - 7, 8)
            for i in range(pieces):
                copy = pltpu.make_async_copy(
                    wide.at[i, :, rows, :],
                    basis_ref.at[:, rows, pl.ds(i * LANES, LANES)],
                    sems.at[x // 8, i],
                )
                copy.start()
                copies.append(copy)
    out_upper_ref[...] = jnp.dot(
        second, upper_ref[...], precision=lax.Precision.HIGHEST, preferred_element_type=F32
    ) * (1.0 / scale)
    for copy in copies:
        copy.wait()


def per_device(vectors, reaction):
    k, nx, plane = vectors.shape
    n_sfc, n_sub = lax.axis_size("sfc"), lax.axis_size("sub")
    table = jnp.asarray(plane_table(NY, NL), BF16)
    scale = math.sqrt(n_sfc * n_sub * nx * plane)
    vmem = pl.BlockSpec(memory_space=pltpu.VMEM)
    anywhere = pl.BlockSpec(memory_space=pl.ANY)
    dma = pltpu.SemaphoreType.DMA
    halo = POWERS * k + 8
    q, upper, gram = pl.pallas_call(
        main_kernel,
        out_shape=(
            jax.ShapeDtypeStruct((nx, k, plane), F32),
            jax.ShapeDtypeStruct((k, k), F32),
            jax.ShapeDtypeStruct((k // 2, 2 * k), F32),
        ),
        in_specs=[anywhere, anywhere, vmem],
        out_specs=(vmem, vmem, vmem),
        scratch_shapes=[
            pltpu.VMEM((plane // LANES, k, nx, LANES), F32),
            pltpu.VMEM((nx + 16, plane), F32),
            pltpu.VMEM((POWERS + 1, nx + 2 * POWERS, k, plane), F32),
            pltpu.VMEM((POWERS, nx + 2 * POWERS, k, plane), F32),
            pltpu.VMEM((halo, plane), F32),
            pltpu.VMEM((halo, plane), F32),
            pltpu.VMEM((halo, plane), F32),
            pltpu.VMEM((halo, plane), F32),
            pltpu.VMEM((n_sub, k // 2, 2 * k), F32),
            pltpu.VMEM((n_sfc, k // 2, 2 * k), F32),
            pltpu.VMEM((n_sub, k // 2, 2 * k), F32),
            pltpu.VMEM((n_sfc, k // 2, 2 * k), F32),
            dma((plane // LANES + 1,)),
            dma((2,)),
            dma((2,)),
            dma((n_sub,)),
            dma((n_sub,)),
            dma((n_sfc,)),
            dma((n_sfc,)),
            dma((n_sub,)),
            dma((n_sub,)),
            dma((n_sfc,)),
            dma((n_sfc,)),
        ],
        compiler_params=pltpu.CompilerParams(
            collective_id=0, has_side_effects=True, vmem_limit_bytes=48 * 1024 * 1024
        ),
        name="power_gram_factor",
    )(vectors, reaction, table)
    basis, upper = pl.pallas_call(
        functools.partial(last_kernel, scale),
        out_shape=(
            jax.ShapeDtypeStruct((k, nx, plane), F32),
            jax.ShapeDtypeStruct((k, k), F32),
        ),
        in_specs=[vmem, vmem, vmem],
        out_specs=(anywhere, vmem),
        scratch_shapes=[
            pltpu.VMEM((plane // LANES, k, nx, LANES), F32),
            dma((nx // 8, plane // LANES)),
        ],
        compiler_params=pltpu.CompilerParams(vmem_limit_bytes=32 * 1024 * 1024),
        name="second_factor",
    )(q, upper, gram)
    return basis, upper


def solution(mesh):
    placed = (P(None, ("sfc", "sub"), None), P(("sfc", "sub"), None))
    return jax.shard_map(
        per_device,
        mesh=mesh,
        in_specs=placed,
        out_specs=(P(None, ("sfc", "sub"), None), P()),
        check_vma=False,
    )
```

```python
import functools
import math

import jax
import jax.numpy as jnp
import numpy as np
from jax import lax
from jax.experimental import pallas as pl
from jax.experimental.pallas import tpu as pltpu
from jax.sharding import PartitionSpec as P

NY = 32
NL = 8
POWERS = 3

MESH = pl.DeviceIdType.MESH
F32 = jnp.float32
BF16 = jnp.bfloat16
STEP = 16
LANES = 128
VMEM_ALL = 67043328


def plane_table(across, layers):
    def near(n):
        return np.eye(n, k=1) + np.eye(n, k=-1)

    one_a, one_l = np.eye(across), np.eye(layers)
    same = np.kron(one_l, one_a)
    side = np.kron(one_l, near(across)) + np.kron(near(layers), one_a)
    corner = np.kron(near(layers), near(across))
    edge = 16.0 * same - 68.0 * side - 35.0 * corner
    own = 304.0 * same + 4.0 * side - 17.0 * corner
    return np.concatenate([edge, own], axis=1)


def split3(x):
    high = x.astype(BF16)
    rest = x - high.astype(F32)
    mid = rest.astype(BF16)
    low = (rest - mid.astype(F32)).astype(BF16)
    return high, mid, low


def loop(count, body):
    if count <= 16:
        for i in range(count):
            body(i)
    else:
        lax.fori_loop(0, count, lambda i, c: (body(i), c)[1], 0)


def gram_of(slabs):
    k = slabs[0].shape[0]
    wide = jnp.concatenate([jnp.concatenate(split3(s), axis=0) for s in slabs], axis=1)
    pairs = lax.dot_general(wide, wide, (((1,), (1,)), ((), ())), preferred_element_type=F32)
    total = None
    for i in (2, 1, 0):
        for j in (2, 1, 0):
            term = pairs[i * k : (i + 1) * k, j * k : (j + 1) * k]
            total = term if total is None else total + term
    return total


def left_parts(matrix):
    a, b, c = split3(matrix)
    return jnp.concatenate([a, a, a, b, b, c], axis=1)


def left_apply(parts, slab):
    a, b, c = split3(slab)
    stacked = jnp.concatenate([a, b, c, a, b, a], axis=0)
    return jnp.dot(parts, stacked, preferred_element_type=F32)


def eliminate(gram):
    k = gram.shape[0]
    rows = lax.broadcasted_iota(jnp.int32, (k, 2 * k), 0)
    cols = lax.broadcasted_iota(jnp.int32, (k, 2 * k), 1)
    unit = (rows + k == cols).astype(F32)
    work = jnp.concatenate([gram, unit[:, k:]], axis=1)
    for start in range(0, k, STEP):
        base = start // 8 * 8
        done, live = work[:base], work[base:]
        live_rows = rows[base:]
        n = live.shape[0]
        columns = [jnp.broadcast_to(live[:, start + i : start + i + 1], (n, 2 * k)) for i in range(STEP)]
        for i in range(STEP):
            j = start + i
            at = j - base
            pivot = columns[i][at : at + 1, :]
            factor = jnp.where(live_rows > j, columns[i] * (1.0 / pivot), 0.0)
            for later in range(i + 1, STEP):
                columns[later] = columns[later] - factor * columns[later][at : at + 1, :]
            live = live - factor * live[at : at + 1, :]
        work = live if base == 0 else jnp.concatenate([done, live], axis=0)
    diagonal = jnp.sum(jnp.where(rows == cols, work, 0.0), axis=1, keepdims=True)
    root = lax.rsqrt(diagonal)
    root = root * (1.5 - 0.5 * diagonal * root * root)
    upper = jnp.where(cols >= rows, work, 0.0)[:, :k] * (1.0 / (diagonal * root))
    inverse = work[:, k:] * root
    return upper, inverse


def square(size):
    rows = lax.broadcasted_iota(jnp.int32, (size, size), 0)
    return rows, lax.broadcasted_iota(jnp.int32, (size, size), 1)


def pack(gram):
    half = gram.shape[0] // 2
    rows, cols = square(half)
    first, cross, second = gram[:half, :half], gram[:half, half:], gram[half:, half:]
    tall = jnp.concatenate([jnp.where(rows >= cols, first, second), cross], axis=1)
    diagonal = jnp.sum(jnp.where(rows == cols, second, 0.0), axis=0, keepdims=True)
    wide = jnp.concatenate([tall[: half // 2], tall[half // 2 :]], axis=1)
    rest = jnp.concatenate([diagonal, jnp.zeros((1, 3 * half), F32)], axis=1)
    return jnp.concatenate([wide, rest], axis=0)


def unpack(packed):
    k = packed.shape[1] // 2
    half = k // 2
    rows, cols = square(half)
    wide = packed[: half // 2]
    tall = jnp.concatenate([wide[:, :k], wide[:, k:]], axis=0)
    turned = tall.T
    both, cross = tall[:, :half], tall[:, half:]
    first = jnp.where(rows >= cols, both, turned[:half])
    diagonal = packed[half // 2 : half // 2 + 1, :half]
    second = jnp.where(rows < cols, both, jnp.where(rows > cols, turned[:half], diagonal))
    return jnp.concatenate(
        [jnp.concatenate([first, cross], axis=1), jnp.concatenate([turned[half:], second], axis=1)], axis=0
    )


def gather_sum(axis, box, send_sem, recv_sem, value):
    count = lax.axis_size(axis)
    me = lax.axis_index(axis)
    sent = pl.ds(0, value.shape[0])
    box[me, sent] = value

    def copy(i, slot, target):
        return pltpu.make_async_remote_copy(
            src_ref=box.at[slot, sent],
            dst_ref=box.at[slot, sent],
            send_sem=send_sem.at[i],
            recv_sem=recv_sem.at[slot],
            device_id={axis: target},
            device_id_type=MESH,
        )

    def start(i):
        copy(i, me, lax.rem(me + i + 1, count)).start()

    def take(i):
        other = lax.rem(me + i + 1, count)
        copy(i, other, other).wait_recv()

    def finish(i):
        copy(i, me, lax.rem(me + i + 1, count)).wait_send()

    loop(count - 1, start)
    loop(count - 1, take)
    if count <= 16:
        total = box[0, sent]
        for i in range(1, count):
            total = total + box[i, sent]
    else:
        total = lax.fori_loop(1, count, lambda i, t: t + box[i, sent], box[0, sent])
    return total, lambda: loop(count - 1, finish)


def main_kernel(
    vec_ref, react_ref, table_ref, q_ref, upper_ref, gram_ref,
    raw, react, coefficients, fields, edges, send_l, send_r, from_l, from_r,
    box_sub1, box_sfc1, box_sub2, box_sfc2,
    upper_buf, in_sem, out_sem, halo_send, halo_recv,
    ss1, rs1, sf1, rf1, ss2, rs2, sf2, rf2,
):
    width = POWERS
    n_sfc, n_sub = lax.axis_size("sfc"), lax.axis_size("sub")
    p_sfc, p_sub = lax.axis_index("sfc"), lax.axis_index("sub")
    me = p_sfc * n_sub + p_sub
    last = n_sfc * n_sub - 1
    k, nx, plane = vec_ref.shape

    lanes = raw.shape[-1]
    loads = [
        pltpu.make_async_copy(vec_ref.at[:, :, pl.ds(i * lanes, lanes)], raw.at[i], in_sem.at[i])
        for i in range(plane // lanes)
    ]
    loads.append(
        pltpu.make_async_copy(react_ref, react.at[pl.ds(8, nx)], in_sem.at[plane // lanes])
    )
    loads.append(pltpu.make_async_copy(table_ref, coefficients, in_sem.at[plane // lanes + 1]))
    for load in loads:
        load.start()

    def device(index):
        return (lax.div(index, n_sub), lax.rem(index, n_sub))

    has_left, has_right = me > 0, me < last
    barrier = pltpu.get_barrier_semaphore()

    def greet(axis, count, mine):
        def one(i):
            pl.semaphore_signal(
                barrier, inc=1, device_id={axis: lax.rem(mine + i + 1, count)}, device_id_type=MESH
            )

        loop(count - 1, one)

    @pl.when(has_left)
    def _():
        pl.semaphore_signal(barrier, inc=1, device_id=device(me - 1), device_id_type=MESH)

    @pl.when(has_right)
    def _():
        pl.semaphore_signal(barrier, inc=1, device_id=device(me + 1), device_id_type=MESH)

    greet("sub", n_sub, p_sub)
    greet("sfc", n_sfc, p_sfc)

    for load in loads[:-1]:
        load.wait()
    flats = [raw.at[i].reshape(k * nx, lanes) for i in range(plane // lanes)]

    def slab(x):
        return jnp.concatenate([flat[pl.ds(x, k, stride=nx), :] for flat in flats], axis=1)

    halo = width * k
    for i in range(width):
        send_l[pl.ds(i * k, k), :] = slab(i)
        send_r[pl.ds(i * k, k), :] = slab(nx - width + i)
    send_l[pl.ds(halo, 8), :] = react[pl.ds(8, 8), :]
    send_r[pl.ds(halo, 8), :] = react[pl.ds(nx, 8), :]
    for x in range(nx):
        fields[0, width + x] = slab(x)

    pl.semaphore_wait(
        barrier, (n_sub - 1) + (n_sfc - 1) + jnp.minimum(me, 1) + jnp.minimum(last - me, 1)
    )

    def to_left():
        return pltpu.make_async_remote_copy(
            src_ref=send_l, dst_ref=from_r, send_sem=halo_send.at[0], recv_sem=halo_recv.at[1],
            device_id=device(me - 1), device_id_type=MESH,
        )

    def to_right():
        return pltpu.make_async_remote_copy(
            src_ref=send_r, dst_ref=from_l, send_sem=halo_send.at[1], recv_sem=halo_recv.at[0],
            device_id=device(me + 1), device_id_type=MESH,
        )

    @pl.when(has_left)
    def _():
        to_left().start()

    @pl.when(has_right)
    def _():
        to_right().start()

    loads[-1].wait()
    table = coefficients[...]

    def products(p, lo, hi):
        v = fields[p, width + lo : width + hi].reshape((hi - lo) * k, plane)
        a, b, c = split3(v)
        both = (
            jnp.dot(a, table, preferred_element_type=F32)
            + jnp.dot(b, table, preferred_element_type=F32)
            + jnp.dot(c, table, preferred_element_type=F32)
        )
        edges[p, width + lo : width + hi] = (both[:, :plane] * (1.0 / 432.0)).reshape(hi - lo, k, plane)
        own = both[:, plane:] * (1.0 / 108.0)
        gain = react[8 + lo : 8 + hi, :][:, None, :]
        fields[p + 1, width + lo : width + hi] = own.reshape(hi - lo, k, plane) + gain * v.reshape(hi - lo, k, plane)

    def combine(p, x):
        fields[p + 1, width + x] = (
            fields[p + 1, width + x] + edges[p, width + x - 1] + edges[p, width + x + 1]
        )

    for p in range(width):
        products(p, p, nx - p)
        for x in range(p + 1, nx - p - 1):
            combine(p, x)
    inner = gram_of([fields[width, width + x] for x in range(width, nx - width)])

    zero = jnp.zeros((halo + 8, plane), F32)

    @pl.when(has_left)
    def _():
        to_right_in = pltpu.make_async_remote_copy(
            src_ref=send_r, dst_ref=from_l, send_sem=halo_send.at[1], recv_sem=halo_recv.at[0],
            device_id=device(me - 1), device_id_type=MESH,
        )
        to_right_in.wait_recv()

    @pl.when(jnp.logical_not(has_left))
    def _():
        from_l[...] = zero

    @pl.when(has_right)
    def _():
        to_left_in = pltpu.make_async_remote_copy(
            src_ref=send_l, dst_ref=from_r, send_sem=halo_send.at[0], recv_sem=halo_recv.at[1],
            device_id=device(me + 1), device_id_type=MESH,
        )
        to_left_in.wait_recv()

    @pl.when(jnp.logical_not(has_right))
    def _():
        from_r[...] = zero

    for i in range(width):
        fields[0, i] = from_l[pl.ds(i * k, k), :]
        fields[0, width + nx + i] = from_r[pl.ds(i * k, k), :]
    react[pl.ds(0, 8), :] = from_l[pl.ds(halo, 8), :]
    react[pl.ds(8 + nx, 8), :] = from_r[pl.ds(halo, 8), :]

    keep_left = jnp.where(has_left, 1.0, 0.0).astype(F32)
    keep_right = jnp.where(has_right, 1.0, 0.0).astype(F32)
    for p in range(width):
        products(p, p - width, p)
        products(p, nx - p, nx - p + width)
        for x in range(p - width + 1, p + 1):
            combine(p, x)
            mirror = nx - 1 - x
            combine(p, mirror)
            if x < 0:
                fields[p + 1, width + x] = fields[p + 1, width + x] * keep_left
                fields[p + 1, width + mirror] = fields[p + 1, width + mirror] * keep_right

    outer_rows = list(range(width)) + list(range(nx - width, nx))
    gram = inner + gram_of([fields[width, width + x] for x in outer_rows])

    def reduce(gram, box_sub, ss, rs, box_sfc, sf, rf):
        part, sent_a = gather_sum("sub", box_sub, ss, rs, pack(gram))
        total, sent_b = gather_sum("sfc", box_sfc, sf, rf, part)
        return total, (sent_a, sent_b)

    total, sent1 = reduce(gram, box_sub1, ss1, rs1, box_sfc1, sf1, rf1)
    upper, inverse = eliminate(unpack(total))
    upper_buf[...] = upper
    parts = left_parts(inverse)
    for x in range(nx):
        fields[0, width + x] = left_apply(parts, fields[width, width + x])
    gram = gram_of([fields[0, width + x] for x in range(nx)])
    stores = [
        pltpu.make_async_copy(fields.at[0, pl.ds(width, nx)], q_ref, out_sem.at[0]),
        pltpu.make_async_copy(upper_buf, upper_ref, out_sem.at[1]),
    ]
    for store in stores:
        store.start()
    total, sent2 = reduce(gram, box_sub2, ss2, rs2, box_sfc2, sf2, rf2)
    short = gram_ref.shape[0] - total.shape[0]
    gram_ref[...] = jnp.concatenate([total, jnp.zeros((short, total.shape[1]), F32)], axis=0)

    for done in stores:
        done.wait()
    for done in sent1 + sent2:
        done()

    @pl.when(has_left)
    def _():
        to_left().wait_send()

    @pl.when(has_right)
    def _():
        to_right().wait_send()


def last_kernel(scale, q_hbm, upper_hbm, gram_ref, basis_ref, out_upper_ref, q_ref, upper_ref, wide, in_sem, sems):
    nx, k, plane = q_hbm.shape
    loads = [
        pltpu.make_async_copy(q_hbm, q_ref, in_sem.at[0]),
        pltpu.make_async_copy(upper_hbm, upper_ref, in_sem.at[1]),
    ]
    for load in loads:
        load.start()
    second, inverse = eliminate(unpack(gram_ref[...]))
    parts = left_parts(inverse * scale)
    for load in loads:
        load.wait()
    pieces = wide.shape[0]
    flats = [wide.at[i].reshape(k * nx, LANES) for i in range(pieces)]
    copies = []
    for x in range(nx):
        slab = left_apply(parts, q_ref[x])
        for i in range(pieces):
            flats[i][pl.ds(x, k, stride=nx), :] = slab[:, i * LANES : (i + 1) * LANES]
        if x % 8 == 7:
            rows = pl.ds(x - 7, 8)
            for i in range(pieces):
                copy = pltpu.make_async_copy(
                    wide.at[i, :, rows, :],
                    basis_ref.at[:, rows, pl.ds(i * LANES, LANES)],
                    sems.at[x // 8, i],
                )
                copy.start()
                copies.append(copy)
    out_upper_ref[...] = jnp.dot(
        second, upper_ref[...], precision=lax.Precision.HIGHEST, preferred_element_type=F32
    ) * (1.0 / scale)
    for copy in copies:
        copy.wait()


def per_device(vectors, reaction):
    k, nx, plane = vectors.shape
    n_sfc, n_sub = lax.axis_size("sfc"), lax.axis_size("sub")
    table = jnp.asarray(plane_table(NY, NL), BF16)
    scale = math.sqrt(n_sfc * n_sub * nx * plane)
    vmem = pl.BlockSpec(memory_space=pltpu.VMEM)
    hbm = pl.BlockSpec(memory_space=pltpu.HBM)
    dma = pltpu.SemaphoreType.DMA
    halo = POWERS * k + 8
    tall = (k // 4 + 8) // 8 * 8
    room = 4 * tall * 2 * k + 2048
    q, upper, gram = pl.pallas_call(
        main_kernel,
        out_shape=(
            jax.ShapeDtypeStruct((nx, k, plane), F32),
            jax.ShapeDtypeStruct((k, k), F32),
            jax.ShapeDtypeStruct((tall, 2 * k), F32),
        ),
        in_specs=[hbm, hbm, hbm],
        out_specs=(hbm, hbm, vmem),
        scratch_shapes=[
            pltpu.VMEM((plane // LANES, k, nx, LANES), F32),
            pltpu.VMEM((nx + 16, plane), F32),
            pltpu.VMEM(table.shape, BF16),
            pltpu.VMEM((POWERS + 1, nx + 2 * POWERS, k, plane), F32),
            pltpu.VMEM((POWERS, nx + 2 * POWERS, k, plane), F32),
            pltpu.VMEM((halo, plane), F32),
            pltpu.VMEM((halo, plane), F32),
            pltpu.VMEM((halo, plane), F32),
            pltpu.VMEM((halo, plane), F32),
            pltpu.VMEM((n_sub, tall, 2 * k), F32),
            pltpu.VMEM((n_sfc, tall, 2 * k), F32),
            pltpu.VMEM((n_sub, tall, 2 * k), F32),
            pltpu.VMEM((n_sfc, tall, 2 * k), F32),
            pltpu.VMEM((k, k), F32),
            dma((plane // LANES + 2,)),
            dma((2,)),
            dma((2,)),
            dma((2,)),
            dma((n_sub,)),
            dma((n_sub,)),
            dma((n_sfc,)),
            dma((n_sfc,)),
            dma((n_sub,)),
            dma((n_sub,)),
            dma((n_sfc,)),
            dma((n_sfc,)),
        ],
        compiler_params=pltpu.CompilerParams(
            collective_id=0, has_side_effects=True, vmem_limit_bytes=VMEM_ALL - room
        ),
        name="power_gram_factor",
    )(vectors, reaction, table)
    basis, upper = pl.pallas_call(
        functools.partial(last_kernel, scale),
        out_shape=(
            jax.ShapeDtypeStruct((k, nx, plane), F32),
            jax.ShapeDtypeStruct((k, k), F32),
        ),
        in_specs=[hbm, hbm, vmem],
        out_specs=(hbm, vmem),
        scratch_shapes=[
            pltpu.VMEM((nx, k, plane), F32),
            pltpu.VMEM((k, k), F32),
            pltpu.VMEM((plane // LANES, k, nx, LANES), F32),
            dma((2,)),
            dma((nx // 8, plane // LANES)),
        ],
        compiler_params=pltpu.CompilerParams(vmem_limit_bytes=VMEM_ALL - room),
        name="second_factor",
    )(q, upper, gram)
    return basis, upper


def solution(mesh):
    placed = (P(None, ("sfc", "sub"), None), P(("sfc", "sub"), None))
    return jax.shard_map(
        per_device,
        mesh=mesh,
        in_specs=placed,
        out_specs=(P(None, ("sfc", "sub"), None), P()),
        check_vma=False,
    )
```

```python
import functools
import math

import jax
import jax.numpy as jnp
import numpy as np
from jax import lax
from jax.experimental import pallas as pl
from jax.experimental.pallas import tpu as pltpu
from jax.sharding import PartitionSpec as P

NY = 32
NL = 8
POWERS = 3

MESH = pl.DeviceIdType.MESH
F32 = jnp.float32
BF16 = jnp.bfloat16
STEP = 16
LANES = 128
VMEM_ALL = 67043328


def plane_table(across, layers):
    def near(n):
        return np.eye(n, k=1) + np.eye(n, k=-1)

    one_a, one_l = np.eye(across), np.eye(layers)
    same = np.kron(one_l, one_a)
    side = np.kron(one_l, near(across)) + np.kron(near(layers), one_a)
    corner = np.kron(near(layers), near(across))
    edge = 16.0 * same - 68.0 * side - 35.0 * corner
    own = 304.0 * same + 4.0 * side - 17.0 * corner
    return np.concatenate([edge, own], axis=1)


def split3(x):
    high = x.astype(BF16)
    rest = x - high.astype(F32)
    mid = rest.astype(BF16)
    low = (rest - mid.astype(F32)).astype(BF16)
    return high, mid, low


def loop(count, body):
    if count <= 16:
        for i in range(count):
            body(i)
    else:
        lax.fori_loop(0, count, lambda i, c: (body(i), c)[1], 0)


def gram_of(slabs):
    k = slabs[0].shape[0]
    wide = jnp.concatenate([jnp.concatenate(split3(s), axis=0) for s in slabs], axis=1)
    pairs = lax.dot_general(wide, wide, (((1,), (1,)), ((), ())), preferred_element_type=F32)
    total = None
    for i in (2, 1, 0):
        for j in (2, 1, 0):
            term = pairs[i * k : (i + 1) * k, j * k : (j + 1) * k]
            total = term if total is None else total + term
    return total


def left_parts(matrix):
    a, b, c = split3(matrix)
    return jnp.concatenate([a, a, a, b, b, c], axis=1)


def left_apply(parts, slab):
    a, b, c = split3(slab)
    stacked = jnp.concatenate([a, b, c, a, b, a], axis=0)
    return jnp.dot(parts, stacked, preferred_element_type=F32)


def eliminate(gram):
    k = gram.shape[0]
    rows = lax.broadcasted_iota(jnp.int32, (k, 2 * k), 0)
    cols = lax.broadcasted_iota(jnp.int32, (k, 2 * k), 1)
    unit = (rows + k == cols).astype(F32)
    work = jnp.concatenate([gram, unit[:, k:]], axis=1)
    for start in range(0, k, STEP):
        base = start // 8 * 8
        done, live = work[:base], work[base:]
        live_rows = rows[base:]
        n = live.shape[0]
        columns = [jnp.broadcast_to(live[:, start + i : start + i + 1], (n, 2 * k)) for i in range(STEP)]
        for i in range(STEP):
            j = start + i
            at = j - base
            pivot = columns[i][at : at + 1, :]
            factor = jnp.where(live_rows > j, columns[i] * (1.0 / pivot), 0.0)
            for later in range(i + 1, STEP):
                columns[later] = columns[later] - factor * columns[later][at : at + 1, :]
            live = live - factor * live[at : at + 1, :]
        work = live if base == 0 else jnp.concatenate([done, live], axis=0)
    diagonal = jnp.sum(jnp.where(rows == cols, work, 0.0), axis=1, keepdims=True)
    root = lax.rsqrt(diagonal)
    root = root * (1.5 - 0.5 * diagonal * root * root)
    upper = jnp.where(cols >= rows, work, 0.0)[:, :k] * (1.0 / (diagonal * root))
    inverse = work[:, k:] * root
    return upper, inverse


def square(size):
    rows = lax.broadcasted_iota(jnp.int32, (size, size), 0)
    return rows, lax.broadcasted_iota(jnp.int32, (size, size), 1)


def pack(gram):
    half = gram.shape[0] // 2
    rows, cols = square(half)
    first, cross, second = gram[:half, :half], gram[:half, half:], gram[half:, half:]
    tall = jnp.concatenate([jnp.where(rows >= cols, first, second), cross], axis=1)
    diagonal = jnp.sum(jnp.where(rows == cols, second, 0.0), axis=0, keepdims=True)
    wide = jnp.concatenate([tall[: half // 2], tall[half // 2 :]], axis=1)
    rest = jnp.concatenate([diagonal, jnp.zeros((1, 3 * half), F32)], axis=1)
    return jnp.concatenate([wide, rest], axis=0)


def unpack(packed):
    k = packed.shape[1] // 2
    half = k // 2
    rows, cols = square(half)
    wide = packed[: half // 2]
    tall = jnp.concatenate([wide[:, :k], wide[:, k:]], axis=0)
    turned = tall.T
    both, cross = tall[:, :half], tall[:, half:]
    first = jnp.where(rows >= cols, both, turned[:half])
    diagonal = packed[half // 2 : half // 2 + 1, :half]
    second = jnp.where(rows < cols, both, jnp.where(rows > cols, turned[:half], diagonal))
    return jnp.concatenate(
        [jnp.concatenate([first, cross], axis=1), jnp.concatenate([turned[half:], second], axis=1)], axis=0
    )


def gather_sum(axis, box, send_sem, recv_sem, value):
    count = lax.axis_size(axis)
    me = lax.axis_index(axis)
    sent = pl.ds(0, value.shape[0])
    box[me, sent] = value

    def copy(i, slot, target):
        return pltpu.make_async_remote_copy(
            src_ref=box.at[slot, sent],
            dst_ref=box.at[slot, sent],
            send_sem=send_sem.at[i],
            recv_sem=recv_sem.at[slot],
            device_id={axis: target},
            device_id_type=MESH,
        )

    def start(i):
        copy(i, me, lax.rem(me + i + 1, count)).start()

    def take(i):
        other = lax.rem(me + i + 1, count)
        copy(i, other, other).wait_recv()

    def finish(i):
        copy(i, me, lax.rem(me + i + 1, count)).wait_send()

    loop(count - 1, start)
    loop(count - 1, take)
    if count <= 16:
        total = box[0, sent]
        for i in range(1, count):
            total = total + box[i, sent]
    else:
        total = lax.fori_loop(1, count, lambda i, t: t + box[i, sent], box[0, sent])
    return total, lambda: loop(count - 1, finish)


def main_kernel(
    vec_ref, react_ref, table_ref, q_ref, upper_ref, gram_ref,
    raw, react, coefficients, fields, edges, send_l, send_r, from_l, from_r,
    box_sub1, box_sfc1, box_sub2, box_sfc2,
    upper_buf, in_sem, out_sem, halo_send, halo_recv,
    ss1, rs1, sf1, rf1, ss2, rs2, sf2, rf2,
):
    width = POWERS
    n_sfc, n_sub = lax.axis_size("sfc"), lax.axis_size("sub")
    p_sfc, p_sub = lax.axis_index("sfc"), lax.axis_index("sub")
    me = p_sfc * n_sub + p_sub
    last = n_sfc * n_sub - 1
    k, nx, plane = vec_ref.shape

    lanes = raw.shape[-1]
    loads = [
        pltpu.make_async_copy(vec_ref.at[:, :, pl.ds(i * lanes, lanes)], raw.at[i], in_sem.at[i])
        for i in range(plane // lanes)
    ]
    loads.append(
        pltpu.make_async_copy(react_ref, react.at[pl.ds(8, nx)], in_sem.at[plane // lanes])
    )
    loads.append(pltpu.make_async_copy(table_ref, coefficients, in_sem.at[plane // lanes + 1]))
    for load in loads:
        load.start()

    def device(index):
        return (lax.div(index, n_sub), lax.rem(index, n_sub))

    has_left, has_right = me > 0, me < last
    barrier = pltpu.get_barrier_semaphore()

    def greet(axis, count, mine):
        def one(i):
            pl.semaphore_signal(
                barrier, inc=1, device_id={axis: lax.rem(mine + i + 1, count)}, device_id_type=MESH
            )

        loop(count - 1, one)

    @pl.when(has_left)
    def _():
        pl.semaphore_signal(barrier, inc=1, device_id=device(me - 1), device_id_type=MESH)

    @pl.when(has_right)
    def _():
        pl.semaphore_signal(barrier, inc=1, device_id=device(me + 1), device_id_type=MESH)

    greet("sub", n_sub, p_sub)
    greet("sfc", n_sfc, p_sfc)

    for load in loads[:-1]:
        load.wait()
    flats = [raw.at[i].reshape(k * nx, lanes) for i in range(plane // lanes)]

    def slab(x):
        return jnp.concatenate([flat[pl.ds(x, k, stride=nx), :] for flat in flats], axis=1)

    halo = width * k
    for i in range(width):
        send_l[pl.ds(i * k, k), :] = slab(i)
        send_r[pl.ds(i * k, k), :] = slab(nx - width + i)
    send_l[pl.ds(halo, 8), :] = react[pl.ds(8, 8), :]
    send_r[pl.ds(halo, 8), :] = react[pl.ds(nx, 8), :]
    for x in range(nx):
        fields[0, width + x] = slab(x)

    pl.semaphore_wait(
        barrier, (n_sub - 1) + (n_sfc - 1) + jnp.minimum(me, 1) + jnp.minimum(last - me, 1)
    )

    def to_left():
        return pltpu.make_async_remote_copy(
            src_ref=send_l, dst_ref=from_r, send_sem=halo_send.at[0], recv_sem=halo_recv.at[1],
            device_id=device(me - 1), device_id_type=MESH,
        )

    def to_right():
        return pltpu.make_async_remote_copy(
            src_ref=send_r, dst_ref=from_l, send_sem=halo_send.at[1], recv_sem=halo_recv.at[0],
            device_id=device(me + 1), device_id_type=MESH,
        )

    @pl.when(has_left)
    def _():
        to_left().start()

    @pl.when(has_right)
    def _():
        to_right().start()

    loads[-1].wait()
    table = coefficients[...]
    tables = jnp.concatenate([table, table, table], axis=0)

    def products(p, *spans):
        slabs = [fields[p, width + x] for lo, hi in spans for x in range(lo, hi)]
        parts = [split3(v) for v in slabs]
        wide = jnp.concatenate([jnp.concatenate(part, axis=1) for part in parts], axis=0)
        both = jnp.dot(wide, tables, preferred_element_type=F32)
        row = 0
        for lo, hi in spans:
            for x in range(lo, hi):
                piece = both[row * k : (row + 1) * k]
                edges[p, width + x] = piece[:, :plane] * (1.0 / 432.0)
                own = piece[:, plane:] * (1.0 / 108.0)
                fields[p + 1, width + x] = own + react[8 + x : 9 + x, :] * slabs[row]
                row += 1

    def combine(p, x):
        fields[p + 1, width + x] = (
            fields[p + 1, width + x] + edges[p, width + x - 1] + edges[p, width + x + 1]
        )

    for p in range(width):
        products(p, (p, nx - p))
        for x in range(p + 1, nx - p - 1):
            combine(p, x)
    inner = gram_of([fields[width, width + x] for x in range(width, nx - width)])

    zero = jnp.zeros((halo + 8, plane), F32)

    @pl.when(has_left)
    def _():
        to_right_in = pltpu.make_async_remote_copy(
            src_ref=send_r, dst_ref=from_l, send_sem=halo_send.at[1], recv_sem=halo_recv.at[0],
            device_id=device(me - 1), device_id_type=MESH,
        )
        to_right_in.wait_recv()

    @pl.when(jnp.logical_not(has_left))
    def _():
        from_l[...] = zero

    @pl.when(has_right)
    def _():
        to_left_in = pltpu.make_async_remote_copy(
            src_ref=send_l, dst_ref=from_r, send_sem=halo_send.at[0], recv_sem=halo_recv.at[1],
            device_id=device(me + 1), device_id_type=MESH,
        )
        to_left_in.wait_recv()

    @pl.when(jnp.logical_not(has_right))
    def _():
        from_r[...] = zero

    for i in range(width):
        fields[0, i] = from_l[pl.ds(i * k, k), :]
        fields[0, width + nx + i] = from_r[pl.ds(i * k, k), :]
    react[pl.ds(0, 8), :] = from_l[pl.ds(halo, 8), :]
    react[pl.ds(8 + nx, 8), :] = from_r[pl.ds(halo, 8), :]

    keep_left = jnp.where(has_left, 1.0, 0.0).astype(F32)
    keep_right = jnp.where(has_right, 1.0, 0.0).astype(F32)
    for p in range(width):
        products(p, (p - width, p), (nx - p, nx - p + width))
        for x in range(p - width + 1, p + 1):
            combine(p, x)
            mirror = nx - 1 - x
            combine(p, mirror)
            if x < 0:
                fields[p + 1, width + x] = fields[p + 1, width + x] * keep_left
                fields[p + 1, width + mirror] = fields[p + 1, width + mirror] * keep_right

    outer_rows = list(range(width)) + list(range(nx - width, nx))
    gram = inner + gram_of([fields[width, width + x] for x in outer_rows])

    def reduce(gram, box_sub, ss, rs, box_sfc, sf, rf):
        part, sent_a = gather_sum("sub", box_sub, ss, rs, pack(gram))
        total, sent_b = gather_sum("sfc", box_sfc, sf, rf, part)
        return total, (sent_a, sent_b)

    total, sent1 = reduce(gram, box_sub1, ss1, rs1, box_sfc1, sf1, rf1)
    upper, inverse = eliminate(unpack(total))
    upper_buf[...] = upper
    parts = left_parts(inverse)
    for x in range(nx):
        fields[0, width + x] = left_apply(parts, fields[width, width + x])
    gram = gram_of([fields[0, width + x] for x in range(nx)])
    stores = [
        pltpu.make_async_copy(fields.at[0, pl.ds(width, nx)], q_ref, out_sem.at[0]),
        pltpu.make_async_copy(upper_buf, upper_ref, out_sem.at[1]),
    ]
    for store in stores:
        store.start()
    total, sent2 = reduce(gram, box_sub2, ss2, rs2, box_sfc2, sf2, rf2)
    short = gram_ref.shape[0] - total.shape[0]
    gram_ref[...] = jnp.concatenate([total, jnp.zeros((short, total.shape[1]), F32)], axis=0)

    for done in stores:
        done.wait()
    for done in sent1 + sent2:
        done()

    @pl.when(has_left)
    def _():
        to_left().wait_send()

    @pl.when(has_right)
    def _():
        to_right().wait_send()


def last_kernel(scale, q_hbm, upper_hbm, gram_ref, basis_ref, out_upper_ref, q_ref, upper_ref, wide, in_sem, sems):
    nx, k, plane = q_hbm.shape
    loads = [
        pltpu.make_async_copy(q_hbm, q_ref, in_sem.at[0]),
        pltpu.make_async_copy(upper_hbm, upper_ref, in_sem.at[1]),
    ]
    for load in loads:
        load.start()
    second, inverse = eliminate(unpack(gram_ref[...]))
    parts = left_parts(inverse * scale)
    for load in loads:
        load.wait()
    pieces = wide.shape[0]
    flats = [wide.at[i].reshape(k * nx, LANES) for i in range(pieces)]
    copies = []
    for x in range(nx):
        slab = left_apply(parts, q_ref[x])
        for i in range(pieces):
            flats[i][pl.ds(x, k, stride=nx), :] = slab[:, i * LANES : (i + 1) * LANES]
        if x % 8 == 7:
            rows = pl.ds(x - 7, 8)
            for i in range(pieces):
                copy = pltpu.make_async_copy(
                    wide.at[i, :, rows, :],
                    basis_ref.at[:, rows, pl.ds(i * LANES, LANES)],
                    sems.at[x // 8, i],
                )
                copy.start()
                copies.append(copy)
    out_upper_ref[...] = jnp.dot(
        second, upper_ref[...], precision=lax.Precision.HIGHEST, preferred_element_type=F32
    ) * (1.0 / scale)
    for copy in copies:
        copy.wait()


def per_device(vectors, reaction):
    k, nx, plane = vectors.shape
    n_sfc, n_sub = lax.axis_size("sfc"), lax.axis_size("sub")
    table = jnp.asarray(plane_table(NY, NL), BF16)
    scale = math.sqrt(n_sfc * n_sub * nx * plane)
    vmem = pl.BlockSpec(memory_space=pltpu.VMEM)
    hbm = pl.BlockSpec(memory_space=pltpu.HBM)
    dma = pltpu.SemaphoreType.DMA
    halo = POWERS * k + 8
    tall = (k // 4 + 8) // 8 * 8
    room = 4 * tall * 2 * k + 2048
    q, upper, gram = pl.pallas_call(
        main_kernel,
        out_shape=(
            jax.ShapeDtypeStruct((nx, k, plane), F32),
            jax.ShapeDtypeStruct((k, k), F32),
            jax.ShapeDtypeStruct((tall, 2 * k), F32),
        ),
        in_specs=[hbm, hbm, hbm],
        out_specs=(hbm, hbm, vmem),
        scratch_shapes=[
            pltpu.VMEM((plane // LANES, k, nx, LANES), F32),
            pltpu.VMEM((nx + 16, plane), F32),
            pltpu.VMEM(table.shape, BF16),
            pltpu.VMEM((POWERS + 1, nx + 2 * POWERS, k, plane), F32),
            pltpu.VMEM((POWERS, nx + 2 * POWERS, k, plane), F32),
            pltpu.VMEM((halo, plane), F32),
            pltpu.VMEM((halo, plane), F32),
            pltpu.VMEM((halo, plane), F32),
            pltpu.VMEM((halo, plane), F32),
            pltpu.VMEM((n_sub, tall, 2 * k), F32),
            pltpu.VMEM((n_sfc, tall, 2 * k), F32),
            pltpu.VMEM((n_sub, tall, 2 * k), F32),
            pltpu.VMEM((n_sfc, tall, 2 * k), F32),
            pltpu.VMEM((k, k), F32),
            dma((plane // LANES + 2,)),
            dma((2,)),
            dma((2,)),
            dma((2,)),
            dma((n_sub,)),
            dma((n_sub,)),
            dma((n_sfc,)),
            dma((n_sfc,)),
            dma((n_sub,)),
            dma((n_sub,)),
            dma((n_sfc,)),
            dma((n_sfc,)),
        ],
        compiler_params=pltpu.CompilerParams(
            collective_id=0, has_side_effects=True, vmem_limit_bytes=VMEM_ALL - room
        ),
        name="power_gram_factor",
    )(vectors, reaction, table)
    basis, upper = pl.pallas_call(
        functools.partial(last_kernel, scale),
        out_shape=(
            jax.ShapeDtypeStruct((k, nx, plane), F32),
            jax.ShapeDtypeStruct((k, k), F32),
        ),
        in_specs=[hbm, hbm, vmem],
        out_specs=(hbm, vmem),
        scratch_shapes=[
            pltpu.VMEM((nx, k, plane), F32),
            pltpu.VMEM((k, k), F32),
            pltpu.VMEM((plane // LANES, k, nx, LANES), F32),
            dma((2,)),
            dma((nx // 8, plane // LANES)),
        ],
        compiler_params=pltpu.CompilerParams(vmem_limit_bytes=VMEM_ALL - room),
        name="second_factor",
    )(q, upper, gram)
    return basis, upper


def solution(mesh):
    placed = (P(None, ("sfc", "sub"), None), P(("sfc", "sub"), None))
    return jax.shard_map(
        per_device,
        mesh=mesh,
        in_specs=placed,
        out_specs=(P(None, ("sfc", "sub"), None), P()),
        check_vma=False,
    )
```
